32 devices in a mesh: dp: 8 (over y, x, core), proto: 4 (over z).
Axes of the slice: x: 2, y: 2, z: 4, core: 2. Of those that a mesh axis runs over, the one named last changes fastest.
Arguments:
- hidden_states: bfloat16 [64, 256, 2048], P(('dp', 'proto')), may hold values from -15 to 30, as said below
- teacher_feats: bfloat16 [64, 256, 384], P(('dp', 'proto')), may hold values from -25 to 25, as said below
- masks: int32 [64, 32], P(('dp', 'proto')), may hold values from 0 to 255, as said below
- head_weight: bfloat16 [2048, 384], replicated, as said below
- prototypes: bfloat16 [49152, 384], P('proto'), may hold values from -25 to 25, as said below
- center: float32 [49152], P('proto'), may hold values from -1.8 to 1.8
Outputs:
- loss: float32 [], replicated
- grad_hidden: bfloat16 [2048, 2048], P(('dp', 'proto'))
- grad_head: float32 [2048, 384], P(('dp', 'proto'))
The draws below stay inside these ranges and needn't reach their ends.
Inputs may be any that keep to these rules, and one draw needn't show every extreme that they name: `masks`: each row lists 32 different patch numbers of its image. `hidden_states`: independent entries. `teacher_feats`: independent entries. `head_weight`: independent entries of deviation 2048 ** -0.5. `prototypes`: independent entries.
All inputs are finite; a program needn't handle non-finite values.
Results may differ from the reference program's by a relative error of at most 0.00305.
The reference program's roundings to bfloat16 on the way (of `picked`, `student`, `teacher`, `grads` and `direction`) count: a program that leaves them out, or rounds other values in their place, can miss the bound.
Values may be sent and summed in bfloat16 or wider, within the bound.
No kernel may reach another device: no remote copies, remote signals or barrier semaphores. Data moves between devices by JAX's collectives and lax.ppermute only.
A program may use at most 64 MiB of HBM per device.

```python
import math
import jax
import jax.numpy as jnp
from jax import lax

D_HID = 2048
D_BOT = 384
K = 49152
PATCHES = 256
MASK = 32
IMAGES = 64


def shared_law(key):
    base = jax.random.fold_in(key, 7771)
    weight = jnp.clip(jax.random.normal(jax.random.fold_in(base, 4), (D_HID, D_BOT), jnp.float32), -5.0, 5.0) / math.sqrt(D_HID)
    return weight


def draw_head_weight(key, part):
    return shared_law(key).astype(jnp.bfloat16)


def draw_prototypes(key, part):
    table = 0.2 * jnp.clip(jax.random.normal(jax.random.fold_in(key, 11), (K, D_BOT), jnp.float32), -5.0, 5.0)
    return table.astype(jnp.bfloat16)


def draw_hidden_states(key, part):
    states = jnp.clip(jax.random.normal(jax.random.fold_in(key, 21), (IMAGES, PATCHES, D_HID), jnp.float32), -5.0, 5.0)
    return states.astype(jnp.bfloat16)


def draw_teacher_feats(key, part):
    feats = jnp.clip(jax.random.normal(jax.random.fold_in(key, 31), (IMAGES, PATCHES, D_BOT), jnp.float32), -5.0, 5.0)
    return feats.astype(jnp.bfloat16)


def draw_masks(key, part):
    keys = jax.random.split(jax.random.fold_in(key, 3301), IMAGES)
    return jax.vmap(lambda single: jax.random.permutation(single, PATCHES)[:MASK])(keys).astype(jnp.int32)


def shard_levels(key, dims, pieces, least, high):
    loudness, own = 1.0, jax.random.fold_in(key, 6)
    for dim, parts in pieces:
        draws = jnp.exp(jax.random.uniform(jax.random.fold_in(own, dim), (parts,), jnp.float32, least / len(pieces), high / len(pieces)))
        loudness = loudness * jnp.repeat(draws, dims[dim] // parts).reshape([-1 if axis == dim else 1 for axis in range(len(dims))])
    return loudness


def bell_draw(stream_key, extent, spread, limit, cuts=(), kind=jnp.bfloat16):
    result = jax.random.normal(stream_key, extent, jnp.float32) * spread
    if len(cuts) > 0:
        result = shard_levels(stream_key, extent, cuts, -0.22, 0.18) * result
    return jnp.clip(result, min=-limit, max=limit).astype(kind)


def setup_inputs(seed: int = 0) -> dict:
    arg_keys = jax.random.split(jax.random.key(seed), 7)
    return {
        "hidden_states": draw_hidden_states(jax.random.fold_in(arg_keys[6], 71), 0),
        "teacher_feats": draw_teacher_feats(jax.random.fold_in(arg_keys[6], 71), 0),
        "masks": draw_masks(jax.random.fold_in(arg_keys[6], 71), 0),
        "head_weight": draw_head_weight(jax.random.fold_in(arg_keys[6], 71), 0),
        "prototypes": draw_prototypes(jax.random.fold_in(arg_keys[6], 71), 0),
        "center": bell_draw(arg_keys[5], (K,), 0.3, 1.8, ((0, 4),), jnp.float32),
    }


STUDENT_TEMP = 0.1
TEACHER_TEMP = 0.07
LOSS_SCALE = 524288.0
EPSILON = 1e-06

def unit_rows(feats):
    radius = jnp.sqrt(lax.optimization_barrier(jnp.sum(feats * feats, axis=-1, keepdims=True)) + EPSILON)
    return (feats / radius, radius)

def reference(hidden_states, teacher_feats, masks, head_weight, prototypes, center):
    picked = jnp.take_along_axis(hidden_states, masks[:, :, None], axis=1).reshape(-1, D_HID)
    teacher_rows = jnp.take_along_axis(teacher_feats, masks[:, :, None], axis=1).reshape(-1, D_BOT)
    raw = jnp.dot(picked.astype(jnp.float32), head_weight.astype(jnp.float32))
    unit, radius = unit_rows(raw)
    student = unit.astype(jnp.bfloat16)
    teacher = unit_rows(teacher_rows.astype(jnp.float32))[0].astype(jnp.bfloat16)
    table = prototypes.astype(jnp.float32)
    table_t = table.T
    total_rows = IMAGES * MASK
    factor = LOSS_SCALE / (total_rows * STUDENT_TEMP)
    width = math.gcd(total_rows, 256)

    def one_block(first):
        s_rows = lax.dynamic_slice_in_dim(student, first, width, 0).astype(jnp.float32)
        t_rows = lax.dynamic_slice_in_dim(teacher, first, width, 0).astype(jnp.float32)
        s_logits = jnp.dot(s_rows, table_t) / STUDENT_TEMP
        t_logits = (jnp.dot(t_rows, table_t) - center[None, :]) / TEACHER_TEMP
        peak_s = lax.optimization_barrier(jnp.max(s_logits, axis=1))
        s_weights = jnp.exp(s_logits - peak_s[:, None])
        total_s = lax.optimization_barrier(jnp.sum(s_weights, axis=1))
        peak_t = lax.optimization_barrier(jnp.max(t_logits, axis=1))
        t_weights = jnp.exp(t_logits - peak_t[:, None])
        total_t = lax.optimization_barrier(jnp.sum(t_weights, axis=1))
        cross = lax.optimization_barrier(jnp.sum(t_weights * s_logits, axis=1))
        row_loss = peak_s + jnp.log(total_s) - cross / total_t
        grads = (factor * (s_weights / total_s[:, None] - t_weights / total_t[:, None])).astype(jnp.bfloat16)
        back = jnp.dot(grads.astype(jnp.float32), table)
        return (row_loss, back)
    starts = jnp.arange(total_rows // width, dtype=jnp.int32) * width
    losses, backs = lax.map(one_block, starts)
    back = backs.reshape(total_rows, D_BOT)
    loss = jnp.sum(losses) / total_rows
    inner = lax.optimization_barrier(jnp.sum(unit * back, axis=-1, keepdims=True))
    direction = ((back - unit * inner) / radius).astype(jnp.bfloat16)
    grad_hidden = jnp.dot(direction.astype(jnp.float32), head_weight.astype(jnp.float32).T).astype(jnp.bfloat16)
    grad_head = jnp.dot(picked.astype(jnp.float32).T, direction.astype(jnp.float32))
    return (loss, grad_hidden, grad_head)
```

```python
import functools
import math

import jax
import jax.numpy as jnp
from jax import lax
from jax.experimental import pallas as pl
from jax.experimental.pallas import tpu as pltpu
from jax.sharding import PartitionSpec as P


STUDENT_TEMP = 0.1
TEACHER_TEMP = 0.07
LOSS_SCALE = 524288.0
EPSILON = 1e-06
LOG2E = math.log2(math.e)
LN2 = math.log(2.0)
SCALE_S = LOG2E / STUDENT_TEMP
SCALE_T = LOG2E / TEACHER_TEMP
LANES = 128
NT = (((1,), (1,)), ((), ()))
TN = (((0,), (0,)), ((), ()))
F32 = jnp.float32
BF16 = jnp.bfloat16
VMEM = pl.BlockSpec(memory_space=pltpu.VMEM)
HBM = pl.BlockSpec(memory_space=pltpu.HBM)


def dot(a, b, dims=(((1,), (0,)), ((), ()))):
    return lax.dot_general(a, b, dims, preferred_element_type=F32)


def params(mib):
    return pltpu.CompilerParams(vmem_limit_bytes=mib * 2**20)


def cost(flops, nbytes):
    return pl.CostEstimate(flops=int(flops), bytes_accessed=int(nbytes), transcendentals=0)


def shapes(*specs):
    return tuple(jax.ShapeDtypeStruct(s, d) for s, d in specs)


def pick_kernel(dp, hidden_hbm, feats_hbm, masks_hbm, weight_hbm, rows_out, unit_out, radius_out, *refs):
    cols_out, (hidden, feats, masks, weight, picked_out, sems) = refs[:dp], refs[dp:]
    images, patches, _ = hidden.shape
    fetches = [
        pltpu.make_async_copy(source, target, sems.at[index])
        for index, (source, target) in enumerate(
            [(masks_hbm, masks), (feats_hbm, feats)]
            + [(hidden_hbm.at[image], hidden.at[image]) for image in range(images)]
            + [(weight_hbm, weight)]
        )
    ]
    for fetch in fetches:
        fetch.start()
    fetches[0].wait()
    fetches[1].wait()
    count = masks.shape[1]
    rows = images * count
    patch = lax.broadcasted_iota(jnp.int32, (patches, count), 0)
    for image in range(images):
        here = slice(image * count, (image + 1) * count)
        choice = (patch == masks[image : image + 1, :]).astype(F32).T.astype(BF16)
        fetches[2 + image].wait()
        picked_out[here, :] = dot(choice, hidden[image]).astype(BF16)
        feat = dot(choice, feats[image])
        length = jnp.sqrt(jnp.sum(feat * feat, axis=1, keepdims=True) + EPSILON)
        rows_out[rows + image * count : rows + (image + 1) * count, :] = (feat / length).astype(BF16)
    fetches[2 + images].wait()
    raw = dot(picked_out[...], weight[...])
    radius = jnp.sqrt(jnp.sum(raw * raw, axis=1, keepdims=True) + EPSILON)
    unit = raw / radius
    unit_out[...] = unit
    radius_out[...] = jnp.broadcast_to(radius, radius_out.shape)
    rows_out[0:rows, :] = unit.astype(BF16)
    me = lax.axis_index("dp")
    width = cols_out[0].shape[1]
    for k in range(dp):
        first = pl.multiple_of(jnp.bitwise_xor(me, k) * width, LANES)
        cols_out[k][...] = picked_out[:, pl.ds(first, width)]


def stats_kernel(parts, block, unroll, fetch, *refs):
    inputs = parts + (2 if fetch else 3)
    row_refs, (source, center, *done) = refs[:parts], refs[parts:inputs]
    logits, stats = refs[inputs : inputs + 2]
    protos, scratch = source, refs[inputs + 2 :]
    if fetch:
        protos, sems, *scratch = scratch
    both, tops, sums, cross = scratch
    count = source.shape[0] // block
    ahead = min(3, count)

    def copy(number):
        piece = pl.ds(pl.multiple_of(number * block, block), block)
        return pltpu.make_async_copy(source.at[piece], protos.at[piece], sems.at[number])

    if fetch:
        for number in range(ahead):
            copy(number).start()
    each = row_refs[0].shape[0] // 2
    rows = parts * each
    for index, ref in enumerate(row_refs):
        both[index * each : (index + 1) * each, :] = ref[0:each, :]
        both[rows + index * each : rows + (index + 1) * each, :] = ref[each:, :]
    tops[...] = jnp.full(tops.shape, -jnp.inf, F32)
    sums[...] = jnp.zeros(sums.shape, F32)
    cross[...] = jnp.zeros(cross.shape, F32)
    groups = block // LANES
    chunk = 8

    def project(base, number, u):
        if fetch:
            copy(number + u).wait()
            pl.when(number + u + ahead < count)(lambda: copy(number + u + ahead).start())
        piece = protos[pl.ds(base + u * block, block), :]
        logits[:, pl.ds(base + u * block, block)] = dot(both[...], piece, NT)

    def reduce(base, u):
        lanes = [pl.ds(base + u * block + g * LANES, LANES) for g in range(groups)]
        offset = [center[:, lane] * SCALE_T for lane in lanes]
        for start in range(0, rows, chunk):
            srow = slice(start, start + chunk)
            trow = slice(rows + start, rows + start + chunk)
            s = [logits[srow, lane] * SCALE_S for lane in lanes]
            t = [logits[trow, lane] * SCALE_T - offset[g] for g, lane in enumerate(lanes)]
            old_s, old_t = tops[srow, :], tops[trow, :]
            new_s = functools.reduce(jnp.maximum, s, old_s)
            new_t = functools.reduce(jnp.maximum, t, old_t)
            tops[srow, :] = new_s
            tops[trow, :] = new_t
            fade = jnp.exp2(old_t - new_t)
            e_t = [jnp.exp2(x - new_t) for x in t]
            sums[srow, :] = sums[srow, :] * jnp.exp2(old_s - new_s) + sum(jnp.exp2(x - new_s) for x in s)
            sums[trow, :] = sums[trow, :] * fade + sum(e_t)
            cross[srow, :] = cross[srow, :] * fade + sum(e * x for e, x in zip(e_t, s))

    def step(index, carry):
        base = pl.multiple_of(index * (unroll * block), unroll * block)
        for u in range(unroll):
            project(base, index * unroll, u)
            if u > 0:
                reduce(base, u - 1)
        reduce(base, unroll - 1)
        return carry

    lax.fori_loop(0, count // unroll, step, 0)
    peak = jnp.max(tops[...], axis=1, keepdims=True)
    shrink = jnp.exp2(tops[...] - peak)
    total = jnp.sum(sums[...] * shrink, axis=1, keepdims=True)
    mixed = jnp.sum(cross[...] * shrink[rows:, :], axis=1, keepdims=True)
    lane = lax.broadcasted_iota(jnp.int32, (rows, LANES), 1)
    table = jnp.where(lane == 0, peak[0:rows], 0.0)
    table = jnp.where(lane == 1, total[0:rows], table)
    table = jnp.where(lane == 2, peak[rows:], table)
    table = jnp.where(lane == 3, total[rows:], table)
    table = jnp.where(lane == 4, mixed, table)
    if done:
        stats[:, 0:rows] = done[0][...]
        stats[:, rows:] = table.T[0:8, :]
    else:
        stats[...] = table.T[0:8, :]


def back_kernel(devices, factor, block, parts, which, unroll, *refs):
    stat_refs, (logits, protos, center) = refs[:devices], refs[devices : devices + 3]
    outs = refs[devices + 3 : devices + 3 + parts]
    loss = refs[devices + 3 + parts]
    total, *grads = refs[devices + 4 + parts :]
    rows = logits.shape[0] // 2
    each = rows // parts
    slots = range(which * parts, (which + 1) * parts)
    stats = [
        jnp.concatenate([ref[:, (j ^ k) * each : ((j ^ k) + 1) * each] for j in slots], axis=1)
        for k, ref in enumerate(stat_refs)
    ]
    peak_s = functools.reduce(jnp.maximum, [x[0:1] for x in stats])
    peak_t = functools.reduce(jnp.maximum, [x[2:3] for x in stats])
    sum_s = sum(x[1:2] * jnp.exp2(x[0:1] - peak_s) for x in stats)
    sum_t = sum(x[3:4] * jnp.exp2(x[2:3] - peak_t) for x in stats)
    cross = sum(x[4:5] * jnp.exp2(x[2:3] - peak_t) for x in stats)
    row_loss = LN2 * peak_s + jnp.log(sum_s) - LN2 * (cross / sum_t)
    loss[...] = jnp.broadcast_to(jnp.sum(row_loss, axis=1, keepdims=True), loss.shape)

    def columns(row):
        return jnp.broadcast_to(row, (LANES, rows)).T

    top_s = columns(peak_s + jnp.log2(sum_s * (1.0 / factor)))
    top_t = columns(peak_t + jnp.log2(sum_t * (1.0 / factor)))
    total[...] = jnp.zeros(total.shape, F32)
    groups = block // LANES
    chunk = 16

    def scale(base, u):
        lanes = [pl.ds(base + u * block + g * LANES, LANES) for g in range(groups)]
        for g, lane in enumerate(lanes):
            offset = center[:, lane] * SCALE_T
            for start in range(0, rows, chunk):
                srow = slice(start, start + chunk)
                trow = slice(rows + start, rows + start + chunk)
                value = jnp.exp2(logits[srow, lane] * SCALE_S - top_s[srow])
                value = value - jnp.exp2(logits[trow, lane] * SCALE_T - offset - top_t[srow])
                grads[u][srow, g * LANES : (g + 1) * LANES] = value.astype(BF16)

    def step(index, carry):
        base = pl.multiple_of(index * (unroll * block), unroll * block)
        for u in range(unroll):
            scale(base, u)
            total[...] += dot(grads[u][...], protos[pl.ds(base + u * block, block), :])
        return carry

    lax.fori_loop(0, protos.shape[0] // (block * unroll), step, 0)
    for part in range(parts):
        outs[part][...] = total[part * each : (part + 1) * each, :].astype(outs[part].dtype)


def direction_kernel(devices, halves, *refs):
    backs, (unit, radius), losses, (out,) = (
        refs[:devices],
        refs[devices : devices + 2],
        refs[devices + 2 : devices + 2 + halves],
        refs[devices + 2 + halves :],
    )
    rows = unit.shape[0]
    back = sum(ref[...].astype(F32) for ref in backs)
    inner = jnp.sum(unit[...] * back, axis=1, keepdims=True)
    out[0:rows, :] = ((back - unit[...] * inner) / radius[:, 0:1]).astype(BF16)
    value = jnp.broadcast_to(sum(ref[0:1, 0:1] for ref in losses), (16, out.shape[1]))
    high = value.astype(BF16).astype(F32)
    middle = (value - high).astype(BF16).astype(F32)
    low = value - high - middle
    row = lax.broadcasted_iota(jnp.int32, value.shape, 0)
    out[rows:, :] = jnp.where(row == 0, high, jnp.where(row == 1, middle, low)).astype(BF16)


def hidden_kernel(direction, weight, out):
    rows = out.shape[0]
    out[...] = dot(direction[0:rows, :], weight[...], NT).astype(BF16)


def head_kernel(dp, proto, total_rows, *refs):
    cols, dirs = refs[:dp], refs[dp : 2 * dp]
    outs = refs[2 * dp : 2 * dp + proto]
    loss = refs[2 * dp + proto]
    left, right, result = refs[2 * dp + proto + 1 :]
    rows = cols[0].shape[0]
    value = jnp.zeros((1, LANES), F32)
    for k in range(dp):
        left[k * rows : (k + 1) * rows, :] = cols[k][...]
        right[k * rows : (k + 1) * rows, :] = dirs[k][0:rows, :]
        for term in range(3):
            value = value + dirs[k][rows + term : rows + term + 1, 0:LANES].astype(F32)
    loss[...] = jnp.broadcast_to(value * (1.0 / total_rows), loss.shape)
    result[...] = dot(left[...], right[...], TN)
    me = lax.axis_index("proto")
    size = outs[0].shape[0]
    for k in range(proto):
        first = pl.multiple_of(jnp.bitwise_xor(me, k) * size, 8)
        outs[k][...] = result[pl.ds(first, size), :].astype(outs[k].dtype)


def exchange(x, axis, k):
    size = lax.axis_size(axis)
    return lax.ppermute(x, axis, [(i, i ^ k) for i in range(size)])


def per_device(hidden_states, teacher_feats, masks, head_weight, prototypes, center):
    dp, proto = lax.axis_size("dp"), lax.axis_size("proto")
    assert dp & (dp - 1) == 0 and proto & (proto - 1) == 0
    hid, bot = head_weight.shape
    rows = masks.shape[0] * masks.shape[1]
    local = prototypes.shape[0]
    total_rows = rows * dp * proto
    factor = LOSS_SCALE / (total_rows * STUDENT_TEMP)
    width = hid // dp
    half = proto // 2
    count = half * rows
    block = math.gcd(local, max(LANES, 2**17 // count))
    steps = local // block
    unroll = math.gcd(steps, 6)

    pick = pl.pallas_call(
        functools.partial(pick_kernel, dp),
        out_shape=shapes(
            ((2 * rows, bot), BF16), ((rows, bot), F32), ((rows, LANES), F32),
            *[((rows, width), BF16)] * dp,
        ),
        in_specs=[HBM] * 4,
        out_specs=(VMEM,) * (3 + dp),
        scratch_shapes=[
            pltpu.VMEM(hidden_states.shape, BF16),
            pltpu.VMEM(teacher_feats.shape, BF16),
            pltpu.VMEM(masks.shape, jnp.int32),
            pltpu.VMEM(head_weight.shape, BF16),
            pltpu.VMEM((rows, hid), BF16),
            pltpu.SemaphoreType.DMA((3 + masks.shape[0],)),
        ],
        compiler_params=params(16),
        cost_estimate=cost(2 * rows * hid * bot, hidden_states.size * 2),
        name="pick",
    )(*[pltpu.with_memory_space_constraint(x, pltpu.HBM) for x in (hidden_states, teacher_feats, masks, head_weight)])
    own, unit, radius = pick[:3]
    near = [own] + [exchange(own, "proto", k) for k in range(1, proto)]
    cols = [pick[3]] + [exchange(pick[3 + k], "dp", k) for k in range(1, dp)]

    offsets = center.reshape(1, local)

    def stats_call(parts, table, fetch, *done):
        return pl.pallas_call(
            functools.partial(stats_kernel, half, block, unroll, fetch),
            out_shape=(
                pltpu.VMEM((2 * count, local), F32),
                jax.ShapeDtypeStruct((8, count if fetch else 2 * count), F32),
            ) + ((pltpu.VMEM((local, bot), BF16),) if fetch else ()),
            in_specs=[VMEM] * half + [HBM if fetch else VMEM, VMEM] + [VMEM] * len(done),
            out_specs=(VMEM,) * (3 if fetch else 2),
            scratch_shapes=([pltpu.SemaphoreType.DMA((steps,))] if fetch else []) + [
                pltpu.VMEM((2 * count, bot), BF16),
                pltpu.VMEM((2 * count, LANES), F32),
                pltpu.VMEM((2 * count, LANES), F32),
                pltpu.VMEM((count, LANES), F32),
            ],
            compiler_params=params(6),
            cost_estimate=cost(4 * count * local * bot * 2, local * bot * 2),
            name="stats",
        )(*parts, table, offsets, *done)

    first, sums, table = stats_call(near[:half], pltpu.with_memory_space_constraint(prototypes, pltpu.HBM), True)
    second, mine = stats_call(near[half:], table, False, sums)
    others = [mine] + [exchange(mine, "proto", k) for k in range(1, proto)]

    def back_call(which):
        kinds = [F32] * half
        return pl.pallas_call(
            functools.partial(back_kernel, proto, factor, block, half, which, unroll),
            out_shape=shapes(*[((rows, bot), kind) for kind in kinds], ((8, LANES), F32)),
            in_specs=[VMEM] * (proto + 3),
            out_specs=(VMEM,) * (half + 1),
            scratch_shapes=[pltpu.VMEM((count, bot), F32)] + [pltpu.VMEM((count, block), BF16)] * unroll,
            compiler_params=params(6),
            cost_estimate=cost(2 * count * local * bot * 2, local * bot * 2),
            name="back",
        )(*others, (first, second)[which], table, offsets)

    far = back_call(1)
    close = back_call(0)
    parts = list(close[:half]) + list(far[:half])
    backs = [parts[0]] + [exchange(parts[k], "proto", k) for k in range(1, proto)]

    direction = pl.pallas_call(
        functools.partial(direction_kernel, proto, 2),
        out_shape=jax.ShapeDtypeStruct((rows + 16, bot), BF16),
        in_specs=[VMEM] * (proto + 4),
        out_specs=VMEM,
        compiler_params=params(4),
        cost_estimate=cost(rows * bot * 16, rows * bot * 16),
        name="direction",
    )(*backs, unit, radius, close[half], far[half])
    dirs = [direction] + [exchange(direction, "dp", k) for k in range(1, dp)]
    grad_hidden = pl.pallas_call(
        hidden_kernel,
        out_shape=jax.ShapeDtypeStruct((rows, hid), BF16),
        in_specs=[VMEM] * 2,
        out_specs=VMEM,
        compiler_params=params(8),
        cost_estimate=cost(2 * rows * hid * bot, hid * bot * 2),
        name="hidden",
    )(direction, head_weight)

    size = width // proto
    head = pl.pallas_call(
        functools.partial(head_kernel, dp, proto, total_rows),
        out_shape=shapes(
            *[((size, bot), F32 if k == 0 else BF16) for k in range(proto)], ((8, LANES), F32)
        ),
        in_specs=[VMEM] * (2 * dp),
        out_specs=(VMEM,) * (proto + 1),
        scratch_shapes=[
            pltpu.VMEM((dp * rows, width), BF16),
            pltpu.VMEM((dp * rows, bot), BF16),
            pltpu.VMEM((width, bot), F32),
        ],
        compiler_params=params(8),
        cost_estimate=cost(2 * dp * rows * width * bot, dp * rows * bot * 2),
        name="head",
    )(*cols, *dirs)
    grad_head = head[0]
    for k in range(1, proto):
        grad_head = grad_head + exchange(head[k], "proto", k).astype(F32)
    return (head[proto][0, 0], grad_hidden, grad_head)


def solution(mesh):
    return jax.shard_map(
        per_device,
        mesh=mesh,
        in_specs=(
            P(("dp", "proto"), None, None),
            P(("dp", "proto"), None, None),
            P(("dp", "proto"), None),
            P(),
            P("proto", None),
            P("proto"),
        ),
        out_specs=(P(), P(("dp", "proto"), None), P(("dp", "proto"), None)),
        check_vma=False,
    )
```

```python
import functools
import math

import jax
import jax.numpy as jnp
from jax import lax
from jax.experimental import pallas as pl
from jax.experimental.pallas import tpu as pltpu
from jax.sharding import PartitionSpec as P


STUDENT_TEMP = 0.1
TEACHER_TEMP = 0.07
LOSS_SCALE = 524288.0
EPSILON = 1e-06
LOG2E = math.log2(math.e)
LN2 = math.log(2.0)
SCALE_S = LOG2E / STUDENT_TEMP
SCALE_T = LOG2E / TEACHER_TEMP
LANES = 128
NT = (((1,), (1,)), ((), ()))
TN = (((0,), (0,)), ((), ()))
F32 = jnp.float32
BF16 = jnp.bfloat16
VMEM = pl.BlockSpec(memory_space=pltpu.VMEM)
HBM = pl.BlockSpec(memory_space=pltpu.HBM)


def dot(a, b, dims=(((1,), (0,)), ((), ()))):
    return lax.dot_general(a, b, dims, preferred_element_type=F32)


def params(mib):
    return pltpu.CompilerParams(vmem_limit_bytes=mib * 2**20)


def cost(flops, nbytes):
    return pl.CostEstimate(flops=int(flops), bytes_accessed=int(nbytes), transcendentals=0)


def shapes(*specs):
    return tuple(jax.ShapeDtypeStruct(s, d) for s, d in specs)


def route(devices):
    held, stages, bit = [(k, 0) for k in range(devices)], [], 1
    while bit < devices:
        send = [x for x in held if x[0] & bit]
        keep = [x for x in held if not x[0] & bit]
        stages.append((bit, held, send, keep))
        held = keep + [(k ^ bit, c ^ bit) for k, c in send]
        bit *= 2
    return stages, [c for _, c in held]


def repack(stage, old_keep, arrived, new_send, new_keep):
    _, held, send, keep = stage
    size = old_keep.shape[0] * 2 // len(held)
    for names, target in ((send, new_send), (keep, new_keep)):
        for index, name in enumerate(names):
            place = held.index(name)
            source = old_keep if place < len(held) // 2 else arrived
            place = place % (len(held) // 2)
            target[index * size : (index + 1) * size, :] = source[place * size : (place + 1) * size, :]


def pick_kernel(stage, early, hidden_hbm, feats_hbm, masks_hbm, weight_hbm, center_hbm, protos_hbm, *refs):
    rows_out, unit_out, radius_out, send_out, keep_out, offset_out, protos_out = refs[:7]
    hidden, feats, masks, weight, picked_out, sems = refs[7:]
    images, patches, _ = hidden.shape
    fetches = [
        pltpu.make_async_copy(source, target, sems.at[index])
        for index, (source, target) in enumerate(
            [(masks_hbm, masks), (feats_hbm, feats)]
            + [(hidden_hbm.at[image], hidden.at[image]) for image in range(images)]
            + [(weight_hbm, weight), (center_hbm, offset_out)]
        )
    ]
    for fetch in fetches:
        fetch.start()
    fetches[0].wait()
    fetches[1].wait()
    count = masks.shape[1]
    rows = images * count
    patch = lax.broadcasted_iota(jnp.int32, (patches, count), 0)
    for image in range(images):
        here = slice(image * count, (image + 1) * count)
        choice = (patch == masks[image : image + 1, :]).astype(F32).T.astype(BF16)
        fetches[2 + image].wait()
        picked_out[here, :] = dot(choice, hidden[image]).astype(BF16)
        feat = dot(choice, feats[image])
        length = jnp.sqrt(jnp.sum(feat * feat, axis=1, keepdims=True) + EPSILON)
        rows_out[rows + image * count : rows + (image + 1) * count, :] = (feat / length).astype(BF16)
    fetches[2 + images].wait()
    head = pltpu.make_async_copy(
        protos_hbm.at[pl.ds(0, early)], protos_out.at[pl.ds(0, early)], sems.at[4 + images]
    )
    head.start()
    raw = dot(picked_out[...], weight[...])
    radius = jnp.sqrt(jnp.sum(raw * raw, axis=1, keepdims=True) + EPSILON)
    unit = raw / radius
    unit_out[...] = unit
    radius_out[...] = jnp.broadcast_to(radius, radius_out.shape)
    rows_out[0:rows, :] = unit.astype(BF16)
    me = lax.axis_index("dp")
    _, _, send, keep = stage
    width = send_out.shape[1]
    for names, target in ((send, send_out), (keep, keep_out)):
        for index, (k, _) in enumerate(names):
            first = pl.multiple_of(jnp.bitwise_xor(me, k) * width, LANES)
            target[index * rows : (index + 1) * rows, :] = picked_out[:, pl.ds(first, width)]
    fetches[3 + images].wait()
    offset_out[...] = offset_out[...] * SCALE_T
    head.wait()


def stats_kernel(parts, block, unroll, early, stage, *refs):
    row_refs, refs = refs[:parts], refs[parts:]
    fetch = early is not None
    if fetch:
        protos, offsets, source, logits, stats, protos_out, sems, *scratch = refs
        protos = protos_out
    elif stage:
        protos, offsets, done, keep, arrived, logits, stats, new_send, new_keep, *scratch = refs
        repack(stage, keep, arrived, new_send, new_keep)
    else:
        protos, offsets, done, logits, stats, *scratch = refs
    both, tops, sums, cross = scratch
    count = protos.shape[0] // block
    ready = early // block if fetch else count

    def copy(number):
        first = number * block
        if not isinstance(first, int):
            first = pl.multiple_of(first, block)
        piece = pl.ds(first, block)
        return pltpu.make_async_copy(source.at[piece], protos.at[piece], sems.at[number])

    if fetch:
        for number in range(ready, count):
            copy(number).start()
    each = row_refs[0].shape[0] // 2
    rows = parts * each
    for index, ref in enumerate(row_refs):
        both[index * each : (index + 1) * each, :] = ref[0:each, :]
        both[rows + index * each : rows + (index + 1) * each, :] = ref[each:, :]
    tops[...] = jnp.full(tops.shape, -jnp.inf, F32)
    sums[...] = jnp.zeros(sums.shape, F32)
    cross[...] = jnp.zeros(cross.shape, F32)
    groups = block // LANES
    chunk = 8

    pieces = max(1, block // 256)
    piece = block // pieces

    def project(base, number, u, part):
        if fetch and part == 0:
            current = number + u
            if isinstance(current, int):
                if current >= ready:
                    copy(current).wait()
            else:
                pl.when(current >= ready)(lambda: copy(current).wait())
        columns = pl.ds(base + u * block + part * piece, piece)
        logits[:, columns] = dot(both[...], protos[columns, :], NT)

    def reduce(base, u, part):
        lanes = [pl.ds(base + u * block + g * LANES, LANES) for g in range(groups)]
        offset = [offsets[:, lane] for lane in lanes]
        for start in range(part * rows // pieces, (part + 1) * rows // pieces, chunk):
            srow = slice(start, start + chunk)
            trow = slice(rows + start, rows + start + chunk)
            s = [logits[srow, lane] * SCALE_S for lane in lanes]
            t = [logits[trow, lane] * SCALE_T - offset[g] for g, lane in enumerate(lanes)]
            old_s, old_t = tops[srow, :], tops[trow, :]
            new_s = functools.reduce(jnp.maximum, s, old_s)
            new_t = functools.reduce(jnp.maximum, t, old_t)
            tops[srow, :] = new_s
            tops[trow, :] = new_t
            fade = jnp.exp2(old_t - new_t)
            e_t = [jnp.exp2(x - new_t) for x in t]
            sums[srow, :] = sums[srow, :] * jnp.exp2(old_s - new_s) + sum(jnp.exp2(x - new_s) for x in s)
            sums[trow, :] = sums[trow, :] * fade + sum(e_t)
            cross[srow, :] = cross[srow, :] * fade + sum(e * x for e, x in zip(e_t, s))

    def step(index, carry):
        base = index * (unroll * block)
        if not isinstance(base, int):
            base = pl.multiple_of(base, unroll * block)
        for u in range(unroll + 1):
            for part in range(pieces):
                if u < unroll:
                    project(base, index * unroll, u, part)
                if u > 0:
                    reduce(base, u - 1, part)
        return carry

    if count == unroll:
        step(0, 0)
    else:
        lax.fori_loop(0, count // unroll, step, 0)
    peak = jnp.max(tops[...], axis=1, keepdims=True)
    shrink = jnp.exp2(tops[...] - peak)
    total = jnp.sum(sums[...] * shrink, axis=1, keepdims=True)
    mixed = jnp.sum(cross[...] * shrink[rows:, :], axis=1, keepdims=True)
    lane = lax.broadcasted_iota(jnp.int32, (rows, LANES), 1)
    table = jnp.where(lane == 0, peak[0:rows], 0.0)
    table = jnp.where(lane == 1, total[0:rows], table)
    table = jnp.where(lane == 2, peak[rows:], table)
    table = jnp.where(lane == 3, total[rows:], table)
    table = jnp.where(lane == 4, mixed, table)
    if not fetch:
        stats[:, 0:rows] = done[...]
        stats[:, rows:] = table.T[0:8, :]
    else:
        stats[...] = table.T[0:8, :]


def back_kernel(devices, factor, block, parts, which, unroll, stage, *refs):
    stat_refs, (logits, protos, offsets), refs = refs[:devices], refs[devices : devices + 3], refs[devices + 3 :]
    if stage:
        keep, arrived, *refs = refs
    outs, (loss, *refs) = refs[:parts], refs[parts:]
    if stage:
        new_send, new_keep, *refs = refs
        repack(stage, keep, arrived, new_send, new_keep)
    total, *grads = refs
    rows = logits.shape[0] // 2
    each = rows // parts
    slots = range(which * parts, (which + 1) * parts)
    stats = [
        jnp.concatenate([ref[:, (j ^ k) * each : ((j ^ k) + 1) * each] for j in slots], axis=1)
        for k, ref in enumerate(stat_refs)
    ]
    peak_s = functools.reduce(jnp.maximum, [x[0:1] for x in stats])
    peak_t = functools.reduce(jnp.maximum, [x[2:3] for x in stats])
    sum_s = sum(x[1:2] * jnp.exp2(x[0:1] - peak_s) for x in stats)
    sum_t = sum(x[3:4] * jnp.exp2(x[2:3] - peak_t) for x in stats)
    cross = sum(x[4:5] * jnp.exp2(x[2:3] - peak_t) for x in stats)
    row_loss = LN2 * peak_s + jnp.log(sum_s) - LN2 * (cross / sum_t)
    loss[...] = jnp.broadcast_to(jnp.sum(row_loss, axis=1, keepdims=True), loss.shape)

    def columns(row):
        return jnp.broadcast_to(row, (LANES, rows)).T

    top_s = columns(peak_s + jnp.log2(sum_s * (1.0 / factor)))
    top_t = columns(peak_t + jnp.log2(sum_t * (1.0 / factor)))
    total[...] = jnp.zeros(total.shape, F32)
    groups = block // LANES
    chunk = 16

    def scale(base, u):
        lanes = [pl.ds(base + u * block + g * LANES, LANES) for g in range(groups)]
        for g, lane in enumerate(lanes):
            offset = offsets[:, lane]
            for start in range(0, rows, chunk):
                srow = slice(start, start + chunk)
                trow = slice(rows + start, rows + start + chunk)
                value = jnp.exp2(logits[srow, lane] * SCALE_S - top_s[srow])
                value = value - jnp.exp2(logits[trow, lane] * SCALE_T - offset - top_t[srow])
                grads[u][srow, g * LANES : (g + 1) * LANES] = value.astype(BF16)

    def step(index, carry):
        base = index * (unroll * block)
        if not isinstance(base, int):
            base = pl.multiple_of(base, unroll * block)
        for u in range(unroll + 1):
            if u < unroll:
                scale(base, u)
            if u > 0:
                first = base + (u - 1) * block
                total[...] += dot(grads[u - 1][...], protos[pl.ds(first, block), :])
        return carry

    if protos.shape[0] == block * unroll:
        step(0, 0)
    else:
        lax.fori_loop(0, protos.shape[0] // (block * unroll), step, 0)
    for part in range(parts):
        outs[part][...] = total[part * each : (part + 1) * each, :].astype(outs[part].dtype)


def direction_kernel(devices, halves, stage, *refs):
    backs, (unit, radius), losses, refs = (
        refs[:devices],
        refs[devices : devices + 2],
        refs[devices + 2 : devices + 2 + halves],
        refs[devices + 2 + halves :],
    )
    if stage:
        keep, arrived, out, new_send, new_keep = refs
        repack(stage, keep, arrived, new_send, new_keep)
    else:
        (out,) = refs
    rows = unit.shape[0]
    back = sum(ref[...].astype(F32) for ref in backs)
    inner = jnp.sum(unit[...] * back, axis=1, keepdims=True)
    out[0:rows, :] = ((back - unit[...] * inner) / radius[:, 0:1]).astype(BF16)
    value = jnp.broadcast_to(sum(ref[0:1, 0:1] for ref in losses), (out.shape[0] - rows, out.shape[1]))
    high = value.astype(BF16).astype(F32)
    middle = (value - high).astype(BF16).astype(F32)
    low = value - high - middle
    row = lax.broadcasted_iota(jnp.int32, value.shape, 0)
    out[rows:, :] = jnp.where(row == 0, high, jnp.where(row == 1, middle, low)).astype(BF16)


def hidden_kernel(direction, weight, out):
    rows = out.shape[0]
    out[...] = dot(direction[0:rows, :], weight[...], NT).astype(BF16)


def head_kernel(dp, proto, total_rows, origins, *refs):
    cols, dirs, refs = refs[:2], refs[2 : 2 + dp], refs[2 + dp :]
    outs, (loss, left, right, result) = refs[:proto], refs[proto:]
    rows = cols[0].shape[0] * 2 // dp
    for index, origin in enumerate(origins):
        source = cols[index // (dp // 2)]
        place = index % (dp // 2)
        left[origin * rows : (origin + 1) * rows, :] = source[place * rows : (place + 1) * rows, :]
    value = jnp.zeros((1, LANES), F32)
    for k in range(dp):
        right[k * rows : (k + 1) * rows, :] = dirs[k][0:rows, :]
        for term in range(3):
            value = value + dirs[k][rows + term : rows + term + 1, 0:LANES].astype(F32)
    loss[...] = jnp.broadcast_to(value * (1.0 / total_rows), loss.shape)
    result[...] = dot(left[...], right[...], TN)
    me = lax.axis_index("proto")
    size = outs[0].shape[0]
    for k in range(proto):
        first = pl.multiple_of(jnp.bitwise_xor(me, k) * size, 8)
        outs[k][...] = result[pl.ds(first, size), :].astype(outs[k].dtype)


def exchange(x, axis, k):
    size = lax.axis_size(axis)
    return lax.ppermute(x, axis, [(i, i ^ k) for i in range(size)])


def per_device(hidden_states, teacher_feats, masks, head_weight, prototypes, center):
    dp, proto = lax.axis_size("dp"), lax.axis_size("proto")
    assert dp in (8, 16) and proto & (proto - 1) == 0
    hid, bot = head_weight.shape
    rows = masks.shape[0] * masks.shape[1]
    local = prototypes.shape[0]
    total_rows = rows * dp * proto
    factor = LOSS_SCALE / (total_rows * STUDENT_TEMP)
    width = hid // dp
    half = proto // 2
    count = half * rows
    block = math.gcd(local, max(LANES, 2**17 // count))
    steps = local // block
    unroll = math.gcd(steps, max(1, 12 * 128 // count))

    stages, origins = route(dp)
    moving = jax.ShapeDtypeStruct((dp // 2 * rows, width), BF16)
    early = block * min(4, steps - 1)
    pick = pl.pallas_call(
        functools.partial(pick_kernel, stages[0], early),
        out_shape=(
            *shapes(((2 * rows, bot), BF16), ((rows, bot), F32), ((rows, LANES), F32)),
            moving,
            moving,
            pltpu.VMEM((1, local), F32),
            pltpu.VMEM((local, bot), BF16),
        ),
        in_specs=[HBM] * 6,
        out_specs=(VMEM,) * 7,
        scratch_shapes=[
            pltpu.VMEM(hidden_states.shape, BF16),
            pltpu.VMEM(teacher_feats.shape, BF16),
            pltpu.VMEM(masks.shape, jnp.int32),
            pltpu.VMEM(head_weight.shape, BF16),
            pltpu.VMEM((rows, hid), BF16),
            pltpu.SemaphoreType.DMA((5 + masks.shape[0],)),
        ],
        compiler_params=params(16),
        cost_estimate=cost(2 * rows * hid * bot, hidden_states.size * 2),
        name="pick",
    )
    table = pltpu.with_memory_space_constraint(prototypes, pltpu.HBM)
    sources = (hidden_states, teacher_feats, masks, head_weight, center.reshape(1, local))
    own, unit, radius, send, keep, offsets, protos = pick(
        *[pltpu.with_memory_space_constraint(x, pltpu.HBM) for x in sources], table
    )
    near = [own] + [exchange(own, "proto", k) for k in range(1, proto)]

    def move(number, send, keep):
        stage = stages[number] if number < len(stages) else None
        if number > len(stages):
            return stage, ()
        return stage, (keep, exchange(send, "dp", stages[number - 1][0]))

    def stats_call(parts, early, stage, protos, *more):
        fetch = early is not None
        return pl.pallas_call(
            functools.partial(stats_kernel, half, block, unroll, early, stage),
            out_shape=(
                pltpu.VMEM((2 * count, local), F32),
                jax.ShapeDtypeStruct((8, count if fetch else 2 * count), F32),
            ) + ((pltpu.VMEM((local, bot), BF16),) if fetch else ()) + ((moving,) * 2 if stage else ()),
            in_specs=[VMEM] * (half + 2) + [HBM if fetch else VMEM] + [VMEM] * (len(more) - 1),
            out_specs=(VMEM,) * (2 + fetch + (2 if stage else 0)),
            input_output_aliases={half: 2} if fetch else {},
            scratch_shapes=([pltpu.SemaphoreType.DMA((steps,))] if fetch else []) + [
                pltpu.VMEM((2 * count, bot), BF16),
                pltpu.VMEM((2 * count, LANES), F32),
                pltpu.VMEM((2 * count, LANES), F32),
                pltpu.VMEM((count, LANES), F32),
            ],
            compiler_params=params(6),
            cost_estimate=cost(4 * count * local * bot * 2, local * bot * 2),
            name="stats",
        )(*parts, protos, offsets, *more)

    first, sums, protos = stats_call(near[:half], early, None, protos, table)
    stage, held = move(1, send, keep)
    second, mine, *moved = stats_call(near[half:], None, stage, protos, sums, *(held if stage else ()))
    if stage:
        send, keep = moved
    others = [mine] + [exchange(mine, "proto", k) for k in range(1, proto)]

    def back_call(which, stage, held):
        return pl.pallas_call(
            functools.partial(back_kernel, proto, factor, block, half, which, unroll, stage),
            out_shape=shapes(*[((rows, bot), F32)] * half, ((8, LANES), F32)) + ((moving,) * 2 if stage else ()),
            in_specs=[VMEM] * (proto + 3 + len(held)),
            out_specs=(VMEM,) * (half + 1 + (2 if stage else 0)),
            scratch_shapes=[pltpu.VMEM((count, bot), F32)] + [pltpu.VMEM((count, block), BF16)] * unroll,
            compiler_params=params(6),
            cost_estimate=cost(2 * count * local * bot * 2, local * bot * 2),
            name="back",
        )(*others, (first, second)[which], protos, offsets, *held)

    far = back_call(1, None, ())
    stage, held = move(2, send, keep)
    close = back_call(0, stage, held if stage else ())
    if stage:
        send, keep = close[half + 1 :]
    parts = list(close[:half]) + list(far[:half])
    backs = [parts[0]] + [exchange(parts[k], "proto", k) for k in range(1, proto)]

    stage, last = move(3, send, keep)
    direction = pl.pallas_call(
        functools.partial(direction_kernel, proto, 2, stage),
        out_shape=shapes(((rows + 8, bot), BF16)) + ((moving,) * 2 if stage else ()),
        in_specs=[VMEM] * (proto + 4 + (2 if stage else 0)),
        out_specs=(VMEM,) * (3 if stage else 1),
        compiler_params=params(4),
        cost_estimate=cost(rows * bot * 16, rows * bot * 16),
        name="direction",
    )(*backs, unit, radius, close[half], far[half], *(last if stage else ()))
    if stage:
        _, last = move(4, *direction[1:])
    direction = direction[0]
    dirs = {0: direction}
    dirs.update({k: exchange(direction, "dp", k) for k in range(2, dp, 2)})
    dirs.update({k + 1: exchange(dirs[k], "dp", 1) for k in range(0, dp, 2)})
    grad_hidden = pl.pallas_call(
        hidden_kernel,
        out_shape=jax.ShapeDtypeStruct((rows, hid), BF16),
        in_specs=[VMEM] * 2,
        out_specs=VMEM,
        compiler_params=params(8),
        cost_estimate=cost(2 * rows * hid * bot, hid * bot * 2),
        name="hidden",
    )(direction, head_weight)

    size = width // proto
    head = pl.pallas_call(
        functools.partial(head_kernel, dp, proto, total_rows, origins),
        out_shape=shapes(
            *[((size, bot), F32 if k == 0 else BF16) for k in range(proto)], ((8, LANES), F32)
        ),
        in_specs=[VMEM] * (2 + dp),
        out_specs=(VMEM,) * (proto + 1),
        scratch_shapes=[
            pltpu.VMEM((dp * rows, width), BF16),
            pltpu.VMEM((dp * rows, bot), BF16),
            pltpu.VMEM((width, bot), F32),
        ],
        compiler_params=params(8),
        cost_estimate=cost(2 * dp * rows * width * bot, dp * rows * bot * 2),
        name="head",
    )(*last, *[dirs[k] for k in range(dp)])
    grad_head = head[0]
    for k in range(1, proto):
        grad_head = grad_head + exchange(head[k], "proto", k).astype(F32)
    return (head[proto][0, 0], grad_hidden, grad_head)


def solution(mesh):
    return jax.shard_map(
        per_device,
        mesh=mesh,
        in_specs=(
            P(("dp", "proto"), None, None),
            P(("dp", "proto"), None, None),
            P(("dp", "proto"), None),
            P(),
            P("proto", None),
            P("proto"),
        ),
        out_specs=(P(), P(("dp", "proto"), None), P(("dp", "proto"), None)),
        check_vma=False,
    )
```

```python
import functools
import math

import jax
import jax.numpy as jnp
from jax import lax
from jax.experimental import pallas as pl
from jax.experimental.pallas import tpu as pltpu
from jax.sharding import PartitionSpec as P


STUDENT_TEMP = 0.1
TEACHER_TEMP = 0.07
LOSS_SCALE = 524288.0
EPSILON = 1e-06
LOG2E = math.log2(math.e)
LN2 = math.log(2.0)
SCALE_S = LOG2E / STUDENT_TEMP
SCALE_T = LOG2E / TEACHER_TEMP
LANES = 128
NT = (((1,), (1,)), ((), ()))
TN = (((0,), (0,)), ((), ()))
F32 = jnp.float32
BF16 = jnp.bfloat16
VMEM = pl.BlockSpec(memory_space=pltpu.VMEM)
HBM = pl.BlockSpec(memory_space=pltpu.HBM)


def dot(a, b, dims=(((1,), (0,)), ((), ()))):
    return lax.dot_general(a, b, dims, preferred_element_type=F32)


def params(mib):
    return pltpu.CompilerParams(vmem_limit_bytes=mib * 2**20)


def cost(flops, nbytes):
    return pl.CostEstimate(flops=int(flops), bytes_accessed=int(nbytes), transcendentals=0)


def shapes(*specs):
    return tuple(jax.ShapeDtypeStruct(s, d) for s, d in specs)


def route(devices):
    held, stages, bit = [(k, 0) for k in range(devices)], [], 1
    while bit < devices:
        send = [x for x in held if x[0] & bit]
        keep = [x for x in held if not x[0] & bit]
        stages.append((bit, held, send, keep))
        held = keep + [(k ^ bit, c ^ bit) for k, c in send]
        bit *= 2
    return stages, [c for _, c in held]


def repack(stage, old_keep, arrived, new_send, new_keep):
    _, held, send, keep = stage
    size = old_keep.shape[0] * 2 // len(held)
    for names, target in ((send, new_send), (keep, new_keep)):
        for index, name in enumerate(names):
            place = held.index(name)
            source = old_keep if place < len(held) // 2 else arrived
            place = place % (len(held) // 2)
            target[index * size : (index + 1) * size, :] = source[place * size : (place + 1) * size, :]


def pick_kernel(stage, early, hidden_hbm, feats_hbm, masks_hbm, weight_hbm, center_hbm, protos_hbm, *refs):
    rows_out, unit_out, radius_out, send_out, keep_out, offset_out, protos_out = refs[:7]
    hidden, feats, masks, weight, picked_out, sems = refs[7:]
    images, patches, _ = hidden.shape
    fetches = [
        pltpu.make_async_copy(source, target, sems.at[index])
        for index, (source, target) in enumerate(
            [(masks_hbm, masks), (feats_hbm, feats)]
            + [(hidden_hbm.at[image], hidden.at[image]) for image in range(images)]
            + [(weight_hbm, weight), (center_hbm, offset_out)]
        )
    ]
    for fetch in fetches:
        fetch.start()
    fetches[0].wait()
    fetches[1].wait()
    count = masks.shape[1]
    rows = images * count
    patch = lax.broadcasted_iota(jnp.int32, (patches, count), 0)
    for image in range(images):
        here = slice(image * count, (image + 1) * count)
        choice = (patch == masks[image : image + 1, :]).astype(F32).T.astype(BF16)
        fetches[2 + image].wait()
        picked_out[here, :] = dot(choice, hidden[image]).astype(BF16)
        feat = dot(choice, feats[image])
        length = jnp.sqrt(jnp.sum(feat * feat, axis=1, keepdims=True) + EPSILON)
        rows_out[rows + image * count : rows + (image + 1) * count, :] = (feat / length).astype(BF16)
    head = pltpu.make_async_copy(
        protos_hbm.at[pl.ds(0, early)], protos_out.at[pl.ds(0, early)], sems.at[4 + images]
    )
    head.start()
    fetches[2 + images].wait()
    raw = dot(picked_out[...], weight[...])
    radius = jnp.sqrt(jnp.sum(raw * raw, axis=1, keepdims=True) + EPSILON)
    unit = raw / radius
    unit_out[...] = unit
    radius_out[...] = jnp.broadcast_to(radius, radius_out.shape)
    rows_out[0:rows, :] = unit.astype(BF16)
    me = lax.axis_index("dp")
    _, _, send, keep = stage
    width = send_out.shape[1]
    for names, target in ((send, send_out), (keep, keep_out)):
        for index, (k, _) in enumerate(names):
            first = pl.multiple_of(jnp.bitwise_xor(me, k) * width, LANES)
            target[index * rows : (index + 1) * rows, :] = picked_out[:, pl.ds(first, width)]
    fetches[3 + images].wait()
    offset_out[...] = offset_out[...] * SCALE_T
    head.wait()


def stats_kernel(parts, block, unroll, early, stage, *refs):
    row_refs, refs = refs[:parts], refs[parts:]
    fetch = early is not None
    if fetch:
        protos, offsets, source, logits, stats, protos_out, sems, *scratch = refs
        protos = protos_out
    elif stage:
        protos, offsets, done, keep, arrived, logits, stats, new_send, new_keep, *scratch = refs
        repack(stage, keep, arrived, new_send, new_keep)
    else:
        protos, offsets, done, logits, stats, *scratch = refs
    both, tops, sums, cross = scratch
    count = protos.shape[0] // block
    ready = early // block if fetch else count

    def copy(number):
        first = number * block
        if not isinstance(first, int):
            first = pl.multiple_of(first, block)
        piece = pl.ds(first, block)
        return pltpu.make_async_copy(source.at[piece], protos.at[piece], sems.at[number])

    if fetch:
        for number in range(ready, count):
            copy(number).start()
    each = row_refs[0].shape[0] // 2
    rows = parts * each
    for index, ref in enumerate(row_refs):
        both[index * each : (index + 1) * each, :] = ref[0:each, :]
        both[rows + index * each : rows + (index + 1) * each, :] = ref[each:, :]
    tops[...] = jnp.full(tops.shape, -jnp.inf, F32)
    sums[...] = jnp.zeros(sums.shape, F32)
    cross[...] = jnp.zeros(cross.shape, F32)
    groups = block // LANES
    chunk = 8

    pieces = max(1, block // 256)
    piece = block // pieces

    def project(base, number, u, part):
        if fetch and part == 0:
            current = number + u
            if isinstance(current, int):
                if current >= ready and (current - ready) % 4 == 0:
                    for next_one in range(current, min(current + 4, count)):
                        copy(next_one).wait()
            else:
                pl.when(current >= ready)(lambda: copy(current).wait())
        columns = pl.ds(base + u * block + part * piece, piece)
        logits[:, columns] = dot(both[...], protos[columns, :], NT)

    def reduce(base, u, part):
        lanes = [pl.ds(base + u * block + g * LANES, LANES) for g in range(groups)]
        offset = [offsets[:, lane] for lane in lanes]
        for start in range(part * rows // pieces, (part + 1) * rows // pieces, chunk):
            srow = slice(start, start + chunk)
            trow = slice(rows + start, rows + start + chunk)
            s = [logits[srow, lane] * SCALE_S for lane in lanes]
            t = [logits[trow, lane] * SCALE_T - offset[g] for g, lane in enumerate(lanes)]
            old_s, old_t = tops[srow, :], tops[trow, :]
            new_s = functools.reduce(jnp.maximum, s, old_s)
            new_t = functools.reduce(jnp.maximum, t, old_t)
            tops[srow, :] = new_s
            tops[trow, :] = new_t
            fade = jnp.exp2(old_t - new_t)
            e_t = [jnp.exp2(x - new_t) for x in t]
            sums[srow, :] = sums[srow, :] * jnp.exp2(old_s - new_s) + sum(jnp.exp2(x - new_s) for x in s)
            sums[trow, :] = sums[trow, :] * fade + sum(e_t)
            cross[srow, :] = cross[srow, :] * fade + sum(e * x for e, x in zip(e_t, s))

    def step(index, carry):
        base = index * (unroll * block)
        if not isinstance(base, int):
            base = pl.multiple_of(base, unroll * block)
        for u in range(unroll + 1):
            for part in range(pieces):
                if u < unroll:
                    project(base, index * unroll, u, part)
                if u > 0:
                    reduce(base, u - 1, part)
        return carry

    if count == unroll:
        step(0, 0)
    else:
        lax.fori_loop(0, count // unroll, step, 0)
    peak = jnp.max(tops[...], axis=1, keepdims=True)
    shrink = jnp.exp2(tops[...] - peak)
    total = jnp.sum(sums[...] * shrink, axis=1, keepdims=True)
    mixed = jnp.sum(cross[...] * shrink[rows:, :], axis=1, keepdims=True)
    lane = lax.broadcasted_iota(jnp.int32, (rows, LANES), 1)
    table = jnp.where(lane == 0, peak[0:rows], 0.0)
    table = jnp.where(lane == 1, total[0:rows], table)
    table = jnp.where(lane == 2, peak[rows:], table)
    table = jnp.where(lane == 3, total[rows:], table)
    table = jnp.where(lane == 4, mixed, table)
    if not fetch:
        stats[:, 0:rows] = done[...]
        stats[:, rows:] = table.T[0:8, :]
    else:
        stats[...] = table.T[0:8, :]


def back_kernel(devices, factor, block, parts, which, unroll, stage, *refs):
    stat_refs, (logits, protos, offsets), refs = refs[:devices], refs[devices : devices + 3], refs[devices + 3 :]
    if stage:
        keep, arrived, *refs = refs
    outs, (loss, *refs) = refs[:parts], refs[parts:]
    if stage:
        new_send, new_keep, *refs = refs
        repack(stage, keep, arrived, new_send, new_keep)
    total, *grads = refs
    rows = logits.shape[0] // 2
    each = rows // parts
    slots = range(which * parts, (which + 1) * parts)
    stats = [
        jnp.concatenate([ref[:, (j ^ k) * each : ((j ^ k) + 1) * each] for j in slots], axis=1)
        for k, ref in enumerate(stat_refs)
    ]
    peak_s = functools.reduce(jnp.maximum, [x[0:1] for x in stats])
    peak_t = functools.reduce(jnp.maximum, [x[2:3] for x in stats])
    sum_s = sum(x[1:2] * jnp.exp2(x[0:1] - peak_s) for x in stats)
    sum_t = sum(x[3:4] * jnp.exp2(x[2:3] - peak_t) for x in stats)
    cross = sum(x[4:5] * jnp.exp2(x[2:3] - peak_t) for x in stats)
    row_loss = LN2 * peak_s + jnp.log(sum_s) - LN2 * (cross / sum_t)
    loss[...] = jnp.broadcast_to(jnp.sum(row_loss, axis=1, keepdims=True), loss.shape)

    def columns(row):
        return jnp.broadcast_to(row, (LANES, rows)).T

    top_s = columns(peak_s + jnp.log2(sum_s * (1.0 / factor)))
    top_t = columns(peak_t + jnp.log2(sum_t * (1.0 / factor)))
    total[...] = jnp.zeros(total.shape, F32)
    groups = block // LANES
    chunk = 16

    def scale(base, u):
        lanes = [pl.ds(base + u * block + g * LANES, LANES) for g in range(groups)]
        for g, lane in enumerate(lanes):
            offset = offsets[:, lane]
            for start in range(0, rows, chunk):
                srow = slice(start, start + chunk)
                trow = slice(rows + start, rows + start + chunk)
                value = jnp.exp2(logits[srow, lane] * SCALE_S - top_s[srow])
                value = value - jnp.exp2(logits[trow, lane] * SCALE_T - offset - top_t[srow])
                grads[u][srow, g * LANES : (g + 1) * LANES] = value.astype(BF16)

    def step(index, carry):
        base = index * (unroll * block)
        if not isinstance(base, int):
            base = pl.multiple_of(base, unroll * block)
        for u in range(unroll + 1):
            if u < unroll:
                scale(base, u)
            if u > 0:
                first = base + (u - 1) * block
                total[...] += dot(grads[u - 1][...], protos[pl.ds(first, block), :])
        return carry

    if protos.shape[0] == block * unroll:
        step(0, 0)
    else:
        lax.fori_loop(0, protos.shape[0] // (block * unroll), step, 0)
    for part in range(parts):
        outs[part][...] = total[part * each : (part + 1) * each, :].astype(outs[part].dtype)


def direction_kernel(devices, halves, stage, *refs):
    backs, (unit, radius), losses, refs = (
        refs[:devices],
        refs[devices : devices + 2],
        refs[devices + 2 : devices + 2 + halves],
        refs[devices + 2 + halves :],
    )
    if stage:
        keep, arrived, out, new_send, new_keep = refs
        repack(stage, keep, arrived, new_send, new_keep)
    else:
        (out,) = refs
    rows = unit.shape[0]
    back = sum(ref[...].astype(F32) for ref in backs)
    inner = jnp.sum(unit[...] * back, axis=1, keepdims=True)
    out[0:rows, :] = ((back - unit[...] * inner) / radius[:, 0:1]).astype(BF16)
    value = jnp.broadcast_to(sum(ref[0:1, 0:1] for ref in losses), (out.shape[0] - rows, out.shape[1]))
    high = value.astype(BF16).astype(F32)
    middle = (value - high).astype(BF16).astype(F32)
    low = value - high - middle
    row = lax.broadcasted_iota(jnp.int32, value.shape, 0)
    out[rows:, :] = jnp.where(row == 0, high, jnp.where(row == 1, middle, low)).astype(BF16)


def hidden_kernel(direction, weight, out):
    rows = out.shape[0]
    out[...] = dot(direction[0:rows, :], weight[...], NT).astype(BF16)


def head_kernel(dp, proto, total_rows, origins, *refs):
    cols, dirs, refs = refs[:2], refs[2 : 2 + dp], refs[2 + dp :]
    outs, (loss, left, right, result) = refs[:proto], refs[proto:]
    rows = cols[0].shape[0] * 2 // dp
    for index, origin in enumerate(origins):
        source = cols[index // (dp // 2)]
        place = index % (dp // 2)
        left[origin * rows : (origin + 1) * rows, :] = source[place * rows : (place + 1) * rows, :]
    value = jnp.zeros((1, LANES), F32)
    for k in range(dp):
        right[k * rows : (k + 1) * rows, :] = dirs[k][0:rows, :]
        for term in range(3):
            value = value + dirs[k][rows + term : rows + term + 1, 0:LANES].astype(F32)
    loss[...] = jnp.broadcast_to(value * (1.0 / total_rows), loss.shape)
    result[...] = dot(left[...], right[...], TN)
    me = lax.axis_index("proto")
    size = outs[0].shape[0]
    for k in range(proto):
        first = pl.multiple_of(jnp.bitwise_xor(me, k) * size, 8)
        outs[k][...] = result[pl.ds(first, size), :].astype(outs[k].dtype)


def exchange(x, axis, k):
    size = lax.axis_size(axis)
    return lax.ppermute(x, axis, [(i, i ^ k) for i in range(size)])


def per_device(hidden_states, teacher_feats, masks, head_weight, prototypes, center):
    dp, proto = lax.axis_size("dp"), lax.axis_size("proto")
    assert dp in (8, 16) and proto & (proto - 1) == 0
    hid, bot = head_weight.shape
    rows = masks.shape[0] * masks.shape[1]
    local = prototypes.shape[0]
    total_rows = rows * dp * proto
    factor = LOSS_SCALE / (total_rows * STUDENT_TEMP)
    width = hid // dp
    half = proto // 2
    count = half * rows
    block = math.gcd(local, max(LANES, 2**17 // count))
    steps = local // block
    unroll = math.gcd(steps, max(1, 12 * 128 // count))

    stages, origins = route(dp)
    moving = jax.ShapeDtypeStruct((dp // 2 * rows, width), BF16)
    early = block * min(4, steps - 1)
    pick = pl.pallas_call(
        functools.partial(pick_kernel, stages[0], early),
        out_shape=(
            *shapes(((2 * rows, bot), BF16), ((rows, bot), F32), ((rows, LANES), F32)),
            moving,
            moving,
            pltpu.VMEM((1, local), F32),
            pltpu.VMEM((local, bot), BF16),
        ),
        in_specs=[HBM] * 6,
        out_specs=(VMEM,) * 7,
        scratch_shapes=[
            pltpu.VMEM(hidden_states.shape, BF16),
            pltpu.VMEM(teacher_feats.shape, BF16),
            pltpu.VMEM(masks.shape, jnp.int32),
            pltpu.VMEM(head_weight.shape, BF16),
            pltpu.VMEM((rows, hid), BF16),
            pltpu.SemaphoreType.DMA((5 + masks.shape[0],)),
        ],
        compiler_params=params(16),
        cost_estimate=cost(2 * rows * hid * bot, hidden_states.size * 2),
        name="pick",
    )
    table = pltpu.with_memory_space_constraint(prototypes, pltpu.HBM)
    sources = (hidden_states, teacher_feats, masks, head_weight, center.reshape(1, local))
    own, unit, radius, send, keep, offsets, protos = pick(
        *[pltpu.with_memory_space_constraint(x, pltpu.HBM) for x in sources], table
    )
    near = [own] + [exchange(own, "proto", k) for k in range(1, proto)]

    def move(number, send, keep):
        stage = stages[number] if number < len(stages) else None
        if number > len(stages):
            return stage, ()
        return stage, (keep, exchange(send, "dp", stages[number - 1][0]))

    def stats_call(parts, early, stage, protos, *more):
        fetch = early is not None
        return pl.pallas_call(
            functools.partial(stats_kernel, half, block, unroll, early, stage),
            out_shape=(
                pltpu.VMEM((2 * count, local), F32),
                jax.ShapeDtypeStruct((8, count if fetch else 2 * count), F32),
            ) + ((pltpu.VMEM((local, bot), BF16),) if fetch else ()) + ((moving,) * 2 if stage else ()),
            in_specs=[VMEM] * (half + 2) + [HBM if fetch else VMEM] + [VMEM] * (len(more) - 1),
            out_specs=(VMEM,) * (2 + fetch + (2 if stage else 0)),
            input_output_aliases={half: 2} if fetch else {},
            scratch_shapes=([pltpu.SemaphoreType.DMA((steps,))] if fetch else []) + [
                pltpu.VMEM((2 * count, bot), BF16),
                pltpu.VMEM((2 * count, LANES), F32),
                pltpu.VMEM((2 * count, LANES), F32),
                pltpu.VMEM((count, LANES), F32),
            ],
            compiler_params=params(6),
            cost_estimate=cost(4 * count * local * bot * 2, local * bot * 2),
            name="stats",
        )(*parts, protos, offsets, *more)

    first, sums, protos = stats_call(near[:half], early, None, protos, table)
    stage, held = move(1, send, keep)
    second, mine, *moved = stats_call(near[half:], None, stage, protos, sums, *(held if stage else ()))
    if stage:
        send, keep = moved
    others = [mine] + [exchange(mine, "proto", k) for k in range(1, proto)]

    def back_call(which, stage, held):
        return pl.pallas_call(
            functools.partial(back_kernel, proto, factor, block, half, which, unroll, stage),
            out_shape=shapes(*[((rows, bot), F32)] * half, ((8, LANES), F32)) + ((moving,) * 2 if stage else ()),
            in_specs=[VMEM] * (proto + 3 + len(held)),
            out_specs=(VMEM,) * (half + 1 + (2 if stage else 0)),
            scratch_shapes=[pltpu.VMEM((count, bot), F32)] + [pltpu.VMEM((count, block), BF16)] * unroll,
            compiler_params=params(6),
            cost_estimate=cost(2 * count * local * bot * 2, local * bot * 2),
            name="back",
        )(*others, (first, second)[which], protos, offsets, *held)

    far = back_call(1, None, ())
    stage, held = move(2, send, keep)
    close = back_call(0, stage, held if stage else ())
    if stage:
        send, keep = close[half + 1 :]
    parts = list(close[:half]) + list(far[:half])
    backs = [parts[0]] + [exchange(parts[k], "proto", k) for k in range(1, proto)]

    stage, last = move(3, send, keep)
    direction = pl.pallas_call(
        functools.partial(direction_kernel, proto, 2, stage),
        out_shape=shapes(((rows + 8, bot), BF16)) + ((moving,) * 2 if stage else ()),
        in_specs=[VMEM] * (proto + 4 + (2 if stage else 0)),
        out_specs=(VMEM,) * (3 if stage else 1),
        compiler_params=params(4),
        cost_estimate=cost(rows * bot * 16, rows * bot * 16),
        name="direction",
    )(*backs, unit, radius, close[half], far[half], *(last if stage else ()))
    if stage:
        _, last = move(4, *direction[1:])
    direction = direction[0]
    dirs = {0: direction}
    dirs.update({k: exchange(direction, "dp", k) for k in range(2, dp, 2)})
    dirs.update({k + 1: exchange(dirs[k], "dp", 1) for k in range(0, dp, 2)})
    grad_hidden = pl.pallas_call(
        hidden_kernel,
        out_shape=jax.ShapeDtypeStruct((rows, hid), BF16),
        in_specs=[VMEM] * 2,
        out_specs=VMEM,
        compiler_params=params(8),
        cost_estimate=cost(2 * rows * hid * bot, hid * bot * 2),
        name="hidden",
    )(direction, head_weight)

    size = width // proto
    head = pl.pallas_call(
        functools.partial(head_kernel, dp, proto, total_rows, origins),
        out_shape=shapes(
            *[((size, bot), F32 if k == 0 else BF16) for k in range(proto)], ((8, LANES), F32)
        ),
        in_specs=[VMEM] * (2 + dp),
        out_specs=(VMEM,) * (proto + 1),
        scratch_shapes=[
            pltpu.VMEM((dp * rows, width), BF16),
            pltpu.VMEM((dp * rows, bot), BF16),
            pltpu.VMEM((width, bot), F32),
        ],
        compiler_params=params(8),
        cost_estimate=cost(2 * dp * rows * width * bot, dp * rows * bot * 2),
        name="head",
    )(*last, *[dirs[k] for k in range(dp)])
    grad_head = head[0]
    for k in range(1, proto):
        grad_head = grad_head + exchange(head[k], "proto", k).astype(F32)
    return (head[proto][0, 0], grad_hidden, grad_head)


def solution(mesh):
    return jax.shard_map(
        per_device,
        mesh=mesh,
        in_specs=(
            P(("dp", "proto"), None, None),
            P(("dp", "proto"), None, None),
            P(("dp", "proto"), None),
            P(),
            P("proto", None),
            P("proto"),
        ),
        out_specs=(P(), P(("dp", "proto"), None), P(("dp", "proto"), None)),
        check_vma=False,
    )
```
